32 devices in a mesh: cp: 16 (over z, y, core), vocab: 2 (over x).
Axes of the slice: x: 2, y: 2, z: 4, core: 2. Of those that a mesh axis runs over, the one named last changes fastest.
Arguments:
- queries: bfloat16 [2048, 4096], P('cp', 'vocab'), may hold values from -160 to 160
- key_states: bfloat16 [2048, 1024], P('cp', 'vocab'), may hold values from -6 to 6
- value_states: bfloat16 [2048, 1024], P('cp', 'vocab'), may hold values from -6 to 6
- out_grad: bfloat16 [2048, 4096], P('cp', 'vocab'), may hold values from -6 to 6
- o_weight: bfloat16 [4096, 4096], P('vocab'), may hold values from -0.09375 to 0.09375
- span_order: int32 [32], replicated, may hold values from 0 to 31, each once
Outputs:
- query_grad: float32 [2048, 4096], P('cp', 'vocab')
- key_grad: float32 [2048, 1024], P('cp', 'vocab')
- value_grad: float32 [2048, 1024], P('cp', 'vocab')
The draws below stay inside these ranges and needn't reach their ends.
Inputs may be any that keep to these rules, and one draw needn't show every extreme that they name: `span_order`: each of the 32 span indices once.
All inputs are finite; a program needn't handle non-finite values.
Results may differ from the reference program's by a relative error of at most 0.014.
Values may be sent and summed in bfloat16 or wider, within the bound.
A program may use at most 64 MiB of HBM per device.

```python
import jax
import jax.numpy as jnp
from jax import lax

D = 4096
HEADS = 32
KV_HEADS = 8
HEAD_DIM = 128
TOK_DEV = 128
SEQ = 2048
SPANS = 32


def attention_pair(key):
    base_key = jax.random.fold_in(key, 7101)
    split_keys = jax.random.split(base_key, 2)
    key_values = jnp.clip(jax.random.normal(split_keys[0], (SEQ, KV_HEADS, 1, HEAD_DIM), jnp.float32), -6.0, 6.0)
    query_values = jnp.clip(jax.random.normal(split_keys[1], (SEQ, KV_HEADS, HEADS // KV_HEADS, HEAD_DIM), jnp.float32), -6.0, 6.0)
    return (query_values.reshape(SEQ, HEADS * HEAD_DIM), key_values.reshape(SEQ, KV_HEADS * HEAD_DIM))


def draw_queries(key, part):
    return attention_pair(key)[0].astype(jnp.bfloat16)


def draw_key_states(key, part):
    return attention_pair(key)[1].astype(jnp.bfloat16)


def level_of(own_key, dims, shards, low, largest):
    def one(axis_at, parts):
        steps = jax.random.uniform(jax.random.fold_in(jax.random.fold_in(own_key, 6), axis_at), (parts,), jnp.float32, low / len(shards), largest / len(shards))
        return jnp.repeat(jnp.exp(steps), dims[axis_at] // parts).reshape((-1,) + (1,) * (len(dims) - axis_at - 1))

    gain = one(*shards[0])
    for cut in shards[1:]:
        gain = gain * one(*cut)
    return gain


def bell_draw(rng, dims, scale, limit, pieces=(), held_as=jnp.bfloat16):
    drawn = jax.random.normal(rng, dims, jnp.float32) * scale
    if len(pieces) > 0:
        drawn = level_of(rng, dims, pieces, -0.22, 0.18) * drawn
    return jnp.clip(drawn, min=-limit, max=limit).astype(held_as)


def setup_inputs(seed: int = 0) -> dict:
    key_of = jax.random.split(jax.random.key(seed), 7)
    return {
        "queries": draw_queries(jax.random.fold_in(key_of[6], 71), 0),
        "key_states": draw_key_states(jax.random.fold_in(key_of[6], 71), 0),
        "value_states": bell_draw(key_of[2], (SEQ, KV_HEADS * HEAD_DIM), 1.0, 6.0, ((0, 16), (1, 2))),
        "out_grad": bell_draw(key_of[3], (SEQ, D), 1.0, 6.0, ((0, 16), (1, 2))),
        "o_weight": bell_draw(key_of[4], (HEADS * HEAD_DIM, D), D ** -0.5, 0.09375, ((0, 2),)),
        "span_order": jax.random.permutation(key_of[5], SPANS).astype(jnp.int32),
    }


def positions(span_order, span_rows):
    offsets = jnp.arange(span_rows, dtype=jnp.int32)
    return (span_order.astype(jnp.int32)[:, None] * span_rows + offsets[None, :]).reshape(-1)


def attention_grads(queries, key_states, value_states, upstream, places):
    seq_len = queries.shape[0]
    groups = HEADS // KV_HEADS
    factor = HEAD_DIM ** -0.5
    block_rows = TOK_DEV * 8
    block_count = seq_len // block_rows
    query_heads = queries.reshape(seq_len, KV_HEADS, groups, HEAD_DIM).transpose(1, 2, 0, 3).astype(jnp.float32)
    upstream_heads = upstream.reshape(seq_len, KV_HEADS, groups, HEAD_DIM).transpose(1, 2, 0, 3).astype(jnp.float32)
    key_heads = key_states.reshape(seq_len, KV_HEADS, HEAD_DIM).transpose(1, 0, 2).astype(jnp.float32)
    value_heads = value_states.reshape(seq_len, KV_HEADS, HEAD_DIM).transpose(1, 0, 2).astype(jnp.float32)

    def one_head(operands):
        head_queries, head_upstream, head_keys, head_values = operands

        def block_step(carried, block_index):
            key_total, value_total = carried
            offset = block_index * block_rows
            rows_query = lax.dynamic_slice_in_dim(head_queries, offset, block_rows, 1)
            rows_upstream = lax.dynamic_slice_in_dim(head_upstream, offset, block_rows, 1)
            query_places = lax.dynamic_slice_in_dim(places, offset, block_rows, 0)
            visible = places[None, :] <= query_places[:, None]
            scores = jnp.einsum("gqd,sd->gqs", rows_query, head_keys) * factor
            scores = jnp.where(visible[None], scores, -jnp.inf)
            row_peak = jnp.max(scores, axis=2, keepdims=True)
            logsum = row_peak + jnp.log(jnp.sum(jnp.exp(scores - row_peak), axis=2, keepdims=True))
            weights = jnp.exp(scores - logsum)
            grad_probs = jnp.einsum("gqd,sd->gqs", rows_upstream, head_values)
            deltas = jnp.sum(weights * grad_probs, axis=2, keepdims=True)
            grad_scores = lax.optimization_barrier((weights * (grad_probs - deltas)).astype(jnp.bfloat16)).astype(jnp.float32)
            weights_low = lax.optimization_barrier(weights.astype(jnp.bfloat16)).astype(jnp.float32)
            query_block = jnp.einsum("gqs,sd->gqd", grad_scores, head_keys) * factor
            key_total = key_total + jnp.einsum("gqs,gqd->sd", grad_scores, rows_query) * factor
            value_total = value_total + jnp.einsum("gqs,gqd->sd", weights_low, rows_upstream)
            return (key_total, value_total), query_block

        zeros = jnp.zeros((seq_len, HEAD_DIM), jnp.float32)
        (key_total, value_total), query_stack = lax.scan(block_step, (zeros, zeros), jnp.arange(block_count, dtype=jnp.int32))
        query_total = query_stack.transpose(1, 0, 2, 3).reshape(groups, seq_len, HEAD_DIM)
        return key_total, value_total, query_total

    key_grads, value_grads, query_grads = lax.map(one_head, (query_heads, upstream_heads, key_heads, value_heads))
    query_grad = query_grads.transpose(2, 0, 1, 3).reshape(seq_len, HEADS * HEAD_DIM)
    key_grad = key_grads.transpose(1, 0, 2).reshape(seq_len, KV_HEADS * HEAD_DIM)
    value_grad = value_grads.transpose(1, 0, 2).reshape(seq_len, KV_HEADS * HEAD_DIM)
    return query_grad, key_grad, value_grad


def reference(queries, key_states, value_states, out_grad, o_weight, span_order):
    upstream = lax.dot_general(out_grad, o_weight, (((1,), (1,)), ((), ())), preferred_element_type=jnp.float32).astype(jnp.bfloat16)
    places = positions(span_order, TOK_DEV // 2)
    query_grad, key_grad, value_grad = attention_grads(queries, key_states, value_states, upstream, places)
    return query_grad, key_grad, value_grad
```

```python
import functools

import jax
import jax.numpy as jnp
from jax import lax
from jax.experimental import pallas as pl
from jax.experimental.pallas import tpu as pltpu
from jax.sharding import PartitionSpec as P

HEADS = 32
KV_HEADS = 8
HEAD_DIM = 128


def positions(span_order, span_rows):
    offsets = jnp.arange(span_rows, dtype=jnp.int32)
    return (span_order[:, None] * span_rows + offsets[None, :]).reshape(-1)


def block_scores(query_block, key_block, query_places, key_places, factor):
    scores = (
        jnp.einsum("qkgd,skd->kgqs", query_block, key_block, preferred_element_type=jnp.float32)
        * factor
    )
    visible = key_places[None, :] <= query_places[:, None]
    return jnp.where(visible, scores, -jnp.inf)


def local(queries, key_states, value_states, out_grad, o_weight, span_order):
    own_rows = queries.shape[0]
    kv_width = key_states.shape[1]
    kv_heads = kv_width // HEAD_DIM
    groups = HEADS // KV_HEADS
    factor = HEAD_DIM ** (-0.5)
    upstream = lax.dot_general(
        lax.all_gather(out_grad, "vocab", axis=1, tiled=True),
        o_weight,
        (((1,), (1,)), ((), ())),
        preferred_element_type=jnp.float32,
    ).astype(jnp.bfloat16)
    places = positions(span_order, own_rows // 2)
    seq_len = places.shape[0]
    own_places = lax.dynamic_slice_in_dim(places, lax.axis_index("cp") * own_rows, own_rows, 0)
    query_heads = queries.reshape(own_rows, kv_heads, groups, HEAD_DIM)
    upstream_heads = upstream.reshape(own_rows, kv_heads, groups, HEAD_DIM)
    key_all, value_all = (
        lax.all_gather(key_states, "cp", axis=0, tiled=True),
        lax.all_gather(value_states, "cp", axis=0, tiled=True),
    )
    key_all = key_all.reshape(seq_len, kv_heads, HEAD_DIM)
    value_all = value_all.reshape(seq_len, kv_heads, HEAD_DIM)
    block_rows = own_rows * 8
    block_count = seq_len // block_rows
    block_ids = jnp.arange(block_count, dtype=jnp.int32)
    stat_shape = (kv_heads, groups, own_rows)

    def key_block(block_index):
        offset = block_index * block_rows
        return (
            lax.dynamic_slice_in_dim(key_all, offset, block_rows, 0),
            lax.dynamic_slice_in_dim(value_all, offset, block_rows, 0),
            lax.dynamic_slice_in_dim(places, offset, block_rows, 0),
        )

    def stats_step(carried, block_index):
        running, totals, delta_acc = carried
        keys_now, values_now, places_now = key_block(block_index)
        scores = block_scores(query_heads, keys_now, own_places, places_now, factor)
        newest = jnp.maximum(running, jnp.max(scores, axis=3))
        rescale = jnp.exp(running - newest)
        raised = jnp.exp(scores - newest[..., None])
        grad_probs = jnp.einsum(
            "qkgd,skd->kgqs", upstream_heads, values_now, preferred_element_type=jnp.float32
        )
        totals = totals * rescale + jnp.sum(raised, axis=3)
        delta_acc = delta_acc * rescale + jnp.sum(raised * grad_probs, axis=3)
        return ((newest, totals, delta_acc), None)

    start_stats = (
        jnp.full(stat_shape, -1e30, jnp.float32),
        jnp.zeros(stat_shape, jnp.float32),
        jnp.zeros(stat_shape, jnp.float32),
    )
    (running, totals, delta_acc), unused = lax.scan(stats_step, start_stats, block_ids)
    logsum = running + jnp.log(totals)
    deltas = delta_acc / totals

    def grad_pieces(block_index):
        keys_now, values_now, places_now = key_block(block_index)
        scores = block_scores(query_heads, keys_now, own_places, places_now, factor)
        weights = jnp.exp(scores - logsum[..., None])
        grad_probs = jnp.einsum(
            "qkgd,skd->kgqs", upstream_heads, values_now, preferred_element_type=jnp.float32
        )
        grad_scores = (weights * (grad_probs - deltas[..., None])).astype(jnp.bfloat16)
        return (keys_now, weights, grad_scores)

    query_zeros = jnp.zeros((own_rows, kv_heads, groups, HEAD_DIM), jnp.float32)

    def grad_step(carried, block_index):
        keys_now, weights, grad_scores = grad_pieces(block_index)
        carried = (
            carried
            + jnp.einsum(
                "kgqs,skd->qkgd", grad_scores, keys_now, preferred_element_type=jnp.float32
            )
            * factor
        )
        key_term = (
            jnp.einsum(
                "kgqs,qkgd->skd", grad_scores, query_heads, preferred_element_type=jnp.float32
            )
            * factor
        )
        value_term = jnp.einsum(
            "kgqs,qkgd->skd",
            weights.astype(jnp.bfloat16),
            upstream_heads,
            preferred_element_type=jnp.float32,
        )
        joined = jnp.concatenate(
            (key_term.reshape(block_rows, kv_width), value_term.reshape(block_rows, kv_width)),
            axis=1,
        )
        return (carried, joined)

    query_total, stacked = lax.scan(grad_step, query_zeros, block_ids)
    terms = stacked.reshape(seq_len, 2 * kv_width)
    mine = lax.psum_scatter(
        terms.astype(jnp.bfloat16), "cp", scatter_dimension=0, tiled=True
    ).astype(jnp.float32)
    key_grad = mine[:, :kv_width]
    value_grad = mine[:, kv_width:]
    query_grad = query_total.reshape(own_rows, kv_heads * groups * HEAD_DIM)
    return (query_grad, key_grad, value_grad)


MESH = pl.DeviceIdType.MESH
NT = (((1,), (1,)), ((), ()))
NN = (((1,), (0,)), ((), ()))
TILE = 256


def dot(a, b, dims):
    return lax.dot_general(a, b, dims, preferred_element_type=jnp.float32)


def greet(peers):
    barrier = pltpu.get_barrier_semaphore()
    for peer in peers:
        pl.semaphore_signal(barrier, inc=1, device_id=peer, device_id_type=MESH)
    pl.semaphore_wait(barrier, len(peers))


def send_kernel(
    n, groups, q_ref, k_ref, v_ref, g_ref, w_ref, q_all, k_all, v_all, u_all,
    own_g, other_g, own_w, other_w, partial, u_buf,
    send_sem, recv_sem, own_sem, w_sem, g_sem, gx_sem,
):
    me = lax.axis_index("cp")
    half = lax.axis_index("vocab")
    pairs = n // 2
    width = g_ref.shape[1]
    two = 2 * HEAD_DIM

    def w_copy(t, own):
        pair = lax.rem(me // 2 + t, pairs)
        side = half if own else 1 - half
        return pltpu.make_async_copy(
            w_ref.at[
                pl.ds(pl.multiple_of(pair * two, two), two),
                pl.ds(pl.multiple_of(side * width, width), width),
            ],
            (own_w if own else other_w).at[t],
            w_sem.at[0 if own else 1, t],
        )

    own_g_copy = pltpu.make_async_copy(g_ref, own_g, g_sem)
    own_g_copy.start()
    order = list(range(1, pairs)) + [0]
    for t in order:
        w_copy(t, True).start()
    for t in order:
        w_copy(t, False).start()

    greet([{"cp": lax.rem(me + s, n)} for s in range(1, n)] + [{"vocab": 1 - half}])

    g_copy = pltpu.make_async_remote_copy(
        src_ref=g_ref, dst_ref=other_g, send_sem=gx_sem.at[0], recv_sem=gx_sem.at[1],
        device_id={"vocab": 1 - half}, device_id_type=MESH,
    )
    g_copy.start()

    def head_of(ref, h):
        return ref.at[:, pl.ds(pl.multiple_of(h * HEAD_DIM, HEAD_DIM), HEAD_DIM)]

    def exchange(i, peer, source, target):
        return pltpu.make_async_remote_copy(
            src_ref=source, dst_ref=target.at[me],
            send_sem=send_sem.at[i, peer], recv_sem=recv_sem.at[i, me],
            device_id={"cp": peer}, device_id_type=MESH,
        )

    def input_copies(peer):
        return (
            exchange(0, peer, head_of(q_ref, peer), q_all),
            exchange(1, peer, head_of(k_ref, peer // groups), k_all),
            exchange(2, peer, head_of(v_ref, peer // groups), v_all),
        )

    def send_inputs(s, carry):
        for copy in input_copies(lax.rem(me + s, n)):
            copy.start()
        return carry

    lax.fori_loop(1, n, send_inputs, 0)
    own_copies = (
        pltpu.make_async_copy(head_of(q_ref, me), q_all.at[me], own_sem.at[0]),
        pltpu.make_async_copy(head_of(k_ref, me // groups), k_all.at[me], own_sem.at[1]),
        pltpu.make_async_copy(head_of(v_ref, me // groups), v_all.at[me], own_sem.at[2]),
    )
    for copy in own_copies:
        copy.start()

    own_g_copy.wait()

    def first_half(s, carry):
        t = lax.rem(s, pairs)
        w_copy(t, True).wait()
        partial[t] = dot(own_g[...], own_w[t], NT)
        return carry

    lax.fori_loop(1, pairs + 1, first_half, 0)
    g_copy.wait()

    def finish(t):
        w_copy(t, False).wait()
        u_buf[t] = (partial[t] + dot(other_g[...], other_w[t], NT)).astype(jnp.bfloat16)

    def u_copy(t, peer, side):
        return exchange(3, peer, head_of(u_buf.at[t], side), u_all)

    def second_half(t, carry):
        finish(t)
        base = 2 * lax.rem(me // 2 + t, pairs)
        u_copy(t, base, 0).start()
        u_copy(t, base + 1, 1).start()
        return carry

    lax.fori_loop(1, pairs, second_half, 0)
    finish(0)
    side = lax.rem(me, 2)
    buddy = me + 1 - 2 * side
    u_copy(0, buddy, 1 - side).start()
    own_u = pltpu.make_async_copy(head_of(u_buf.at[0], side), u_all.at[me], own_sem.at[3])
    own_u.start()

    def wait_all(s, carry):
        sent = lax.rem(me + s, n)
        source = lax.rem(me + n - s, n)
        for i, target in enumerate((q_all, k_all, v_all, u_all)):
            done = pltpu.make_async_remote_copy(
                src_ref=target.at[source], dst_ref=target.at[source],
                send_sem=send_sem.at[i, sent], recv_sem=recv_sem.at[i, source],
                device_id={"cp": sent}, device_id_type=MESH,
            )
            done.wait_send()
            done.wait_recv()
        return carry

    lax.fori_loop(1, n, wait_all, 0)
    for copy in own_copies:
        copy.wait()
    own_u.wait()


def attend_kernel(
    order_ref, places_ref, q_ref, k_ref, v_ref, u_ref, dq_out, dkv_out,
    qs, ks, vs, us, k_turned, s_buf, p_buf, dk_sum, dv_sum, dq_sum,
):
    seq = q_ref.shape[0]
    spans = order_ref.shape[0]
    rows = seq // spans
    tiles = seq // TILE
    factor = HEAD_DIM ** (-0.5)
    scale = factor * 1.4426950408889634

    for j in range(spans):
        source = pl.ds(pl.multiple_of(places_ref[j] * rows, rows), rows)
        for target, ref in ((qs, q_ref), (ks, k_ref), (vs, v_ref), (us, u_ref)):
            target[pl.ds(j * rows, rows), :] = ref[source, :]
    k_turned[...] = ks[...].T

    def fold(x, op):
        return op(x.reshape(TILE // 8, 8, TILE), axis=0)

    key_at = lax.broadcasted_iota(jnp.int32, (TILE, TILE), 0)
    query_at = lax.broadcasted_iota(jnp.int32, (TILE, TILE), 1)
    for i in range(tiles):
        own = pl.ds(i * TILE, TILE)
        q_tile = qs[own, :]
        u_tile = us[own, :]
        peak = None
        for j in range(i + 1):
            keys = pl.ds(j * TILE, TILE)
            s = dot(ks[keys, :], q_tile, NT)
            if j == i:
                s = jnp.where(key_at <= query_at, s, -1e30)
            s_buf[keys, :] = s
            top = fold(s, jnp.max)
            peak = top if peak is None else jnp.maximum(peak, top)
        peak = jnp.max(peak, axis=0, keepdims=True)
        total = jnp.zeros((8, TILE), jnp.float32)
        delta = jnp.zeros((8, TILE), jnp.float32)
        for j in range(i + 1):
            keys = pl.ds(j * TILE, TILE)
            p = jnp.exp2((s_buf[keys, :] - peak) * scale)
            dp = dot(vs[keys, :], u_tile, NT)
            total = total + fold(p, jnp.sum)
            delta = delta + fold(p * dp, jnp.sum)
            s_buf[keys, :] = p
            p_buf[keys, :] = dp
        inverse = 1.0 / jnp.sum(total, axis=0, keepdims=True)
        delta = jnp.sum(delta, axis=0, keepdims=True) * inverse
        turned = None
        for j in range(i + 1):
            keys = pl.ds(j * TILE, TILE)
            w = s_buf[keys, :] * inverse
            g = (w * (p_buf[keys, :] - delta)).astype(jnp.bfloat16)
            dk = dot(g, q_tile, NN)
            dv = dot(w.astype(jnp.bfloat16), u_tile, NN)
            if j == i:
                dk_sum[keys, :] = dk
                dv_sum[keys, :] = dv
            else:
                dk_sum[keys, :] += dk
                dv_sum[keys, :] += dv
            part = dot(k_turned[:, keys], g, NN)
            turned = part if turned is None else turned + part
        dq_sum[own, :] = turned.T

    for r in range(spans):
        source = pl.ds(pl.multiple_of(order_ref[r] * rows, rows), rows)
        target = pl.ds(r * rows, rows)
        dq_out[target, :] = (dq_sum[source, :] * factor).astype(jnp.bfloat16)
        dkv_out[target, :HEAD_DIM] = (dk_sum[source, :] * factor).astype(jnp.bfloat16)
        dkv_out[target, HEAD_DIM:] = dv_sum[source, :].astype(jnp.bfloat16)


def return_kernel(n, dq_ref, dkv_ref, dq_all, dkv_all, send_sem, recv_sem, own_sem):
    me = lax.axis_index("cp")
    greet([{"cp": lax.rem(me + s, n)} for s in range(1, n)])
    own_columns = pl.ds(pl.multiple_of(me * HEAD_DIM, HEAD_DIM), HEAD_DIM)

    def copies(s):
        peer = lax.rem(me + s, n)
        return (
            pltpu.make_async_remote_copy(
                src_ref=dkv_ref.at[peer], dst_ref=dkv_all.at[me],
                send_sem=send_sem.at[0, s], recv_sem=recv_sem.at[0, s],
                device_id={"cp": peer}, device_id_type=MESH,
            ),
            pltpu.make_async_remote_copy(
                src_ref=dq_ref.at[peer], dst_ref=dq_all.at[:, own_columns],
                send_sem=send_sem.at[1, s], recv_sem=recv_sem.at[1, s],
                device_id={"cp": peer}, device_id_type=MESH,
            ),
        )

    def start(s, carry):
        for copy in copies(s):
            copy.start()
        return carry

    lax.fori_loop(1, n, start, 0)
    own = (
        pltpu.make_async_copy(dkv_ref.at[me], dkv_all.at[me], own_sem.at[0]),
        pltpu.make_async_copy(dq_ref.at[me], dq_all.at[:, own_columns], own_sem.at[1]),
    )
    for copy in own:
        copy.start()

    def wait(s, carry):
        for copy in copies(s):
            copy.wait()
        return carry

    lax.fori_loop(1, n, wait, 0)
    for copy in own:
        copy.wait()


def by_heads(n, queries, key_states, value_states, out_grad, o_weight, span_order):
    own_rows, width = queries.shape
    kv_heads = key_states.shape[1] // HEAD_DIM
    groups = HEADS // KV_HEADS
    seq = own_rows * n
    pairs = n // 2
    any_spec = pl.BlockSpec(memory_space=pl.ANY)
    vmem_spec = pl.BlockSpec(memory_space=pltpu.VMEM)
    smem_spec = pl.BlockSpec(memory_space=pltpu.SMEM)
    dma = pltpu.SemaphoreType.DMA
    low = jnp.bfloat16
    block = jax.ShapeDtypeStruct((n, own_rows, HEAD_DIM), low)
    gathered = pl.pallas_call(
        functools.partial(send_kernel, n, groups),
        out_shape=(block,) * 4,
        in_specs=[any_spec] * 5,
        out_specs=(vmem_spec,) * 4,
        scratch_shapes=[
            pltpu.VMEM((own_rows, width), low),
            pltpu.VMEM((own_rows, width), low),
            pltpu.VMEM((pairs, 2 * HEAD_DIM, width), low),
            pltpu.VMEM((pairs, 2 * HEAD_DIM, width), low),
            pltpu.VMEM((pairs, own_rows, 2 * HEAD_DIM), jnp.float32),
            pltpu.VMEM((pairs, own_rows, 2 * HEAD_DIM), low),
            dma((4, n)),
            dma((4, n)),
            dma((4,)),
            dma((2, pairs)),
            dma(()),
            dma((2,)),
        ],
        compiler_params=pltpu.CompilerParams(
            collective_id=0, has_side_effects=True, vmem_limit_bytes=40 << 20
        ),
        name="send_heads",
    )(queries, key_states, value_states, out_grad, o_weight)
    spans = span_order.shape[0]
    ids = jnp.arange(spans, dtype=jnp.int32)
    places = jnp.sum(
        jnp.where(span_order[None, :] == ids[:, None], ids[None, :], 0), axis=1, dtype=jnp.int32
    )
    wide = pltpu.VMEM((seq, HEAD_DIM), jnp.float32)
    dq, dkv = pl.pallas_call(
        attend_kernel,
        out_shape=(
            jax.ShapeDtypeStruct((seq, HEAD_DIM), low),
            jax.ShapeDtypeStruct((seq, 2 * HEAD_DIM), low),
        ),
        in_specs=[smem_spec] * 2 + [vmem_spec] * 4,
        out_specs=(vmem_spec,) * 2,
        scratch_shapes=[pltpu.VMEM((seq, HEAD_DIM), low)] * 4
        + [pltpu.VMEM((HEAD_DIM, seq), low)]
        + [pltpu.VMEM((seq, TILE), jnp.float32)] * 2
        + [wide] * 3,
        compiler_params=pltpu.CompilerParams(vmem_limit_bytes=40 << 20),
        name="attend",
    )(span_order, places, *(x.reshape(seq, HEAD_DIM) for x in gathered))
    dq_all, dkv_all = pl.pallas_call(
        functools.partial(return_kernel, n),
        out_shape=(
            jax.ShapeDtypeStruct((own_rows, width), low),
            jax.ShapeDtypeStruct((n, own_rows, 2 * HEAD_DIM), low),
        ),
        in_specs=[any_spec] * 2,
        out_specs=(vmem_spec,) * 2,
        scratch_shapes=[dma((2, n)), dma((2, n)), dma((2,))],
        compiler_params=pltpu.CompilerParams(
            collective_id=1, has_side_effects=True, vmem_limit_bytes=16 << 20
        ),
        name="return_grads",
    )(dq.reshape(n, own_rows, HEAD_DIM), dkv.reshape(n, own_rows, 2 * HEAD_DIM))
    query_grad = dq_all.astype(jnp.float32)

    def over_group(part):
        heads = [
            sum(part[g * groups + h].astype(jnp.float32) for h in range(groups))
            for g in range(kv_heads)
        ]
        return jnp.concatenate(heads, axis=1)

    return (
        query_grad,
        over_group(dkv_all[:, :, :HEAD_DIM]),
        over_group(dkv_all[:, :, HEAD_DIM:]),
    )


def solution(mesh):
    n = mesh.shape["cp"]
    fits = mesh.shape["vocab"] == 2 and HEADS == 2 * n and n % 2 == 0
    body = functools.partial(by_heads, n) if fits else local
    return jax.shard_map(
        body,
        mesh=mesh,
        in_specs=(
            P("cp", "vocab"),
            P("cp", "vocab"),
            P("cp", "vocab"),
            P("cp", "vocab"),
            P("vocab", None),
            P(),
        ),
        out_specs=(P("cp", "vocab"), P("cp", "vocab"), P("cp", "vocab")),
        check_vma=False,
    )
```

```python
import functools

import jax
import jax.numpy as jnp
from jax import lax
from jax.experimental import pallas as pl
from jax.experimental.pallas import tpu as pltpu
from jax.sharding import PartitionSpec as P

HEADS = 32
KV_HEADS = 8
HEAD_DIM = 128


def positions(span_order, span_rows):
    offsets = jnp.arange(span_rows, dtype=jnp.int32)
    return (span_order[:, None] * span_rows + offsets[None, :]).reshape(-1)


def block_scores(query_block, key_block, query_places, key_places, factor):
    scores = (
        jnp.einsum("qkgd,skd->kgqs", query_block, key_block, preferred_element_type=jnp.float32)
        * factor
    )
    visible = key_places[None, :] <= query_places[:, None]
    return jnp.where(visible, scores, -jnp.inf)


def local(queries, key_states, value_states, out_grad, o_weight, span_order):
    own_rows = queries.shape[0]
    kv_width = key_states.shape[1]
    kv_heads = kv_width // HEAD_DIM
    groups = HEADS // KV_HEADS
    factor = HEAD_DIM ** (-0.5)
    upstream = lax.dot_general(
        lax.all_gather(out_grad, "vocab", axis=1, tiled=True),
        o_weight,
        (((1,), (1,)), ((), ())),
        preferred_element_type=jnp.float32,
    ).astype(jnp.bfloat16)
    places = positions(span_order, own_rows // 2)
    seq_len = places.shape[0]
    own_places = lax.dynamic_slice_in_dim(places, lax.axis_index("cp") * own_rows, own_rows, 0)
    query_heads = queries.reshape(own_rows, kv_heads, groups, HEAD_DIM)
    upstream_heads = upstream.reshape(own_rows, kv_heads, groups, HEAD_DIM)
    key_all, value_all = (
        lax.all_gather(key_states, "cp", axis=0, tiled=True),
        lax.all_gather(value_states, "cp", axis=0, tiled=True),
    )
    key_all = key_all.reshape(seq_len, kv_heads, HEAD_DIM)
    value_all = value_all.reshape(seq_len, kv_heads, HEAD_DIM)
    block_rows = own_rows * 8
    block_count = seq_len // block_rows
    block_ids = jnp.arange(block_count, dtype=jnp.int32)
    stat_shape = (kv_heads, groups, own_rows)

    def key_block(block_index):
        offset = block_index * block_rows
        return (
            lax.dynamic_slice_in_dim(key_all, offset, block_rows, 0),
            lax.dynamic_slice_in_dim(value_all, offset, block_rows, 0),
            lax.dynamic_slice_in_dim(places, offset, block_rows, 0),
        )

    def stats_step(carried, block_index):
        running, totals, delta_acc = carried
        keys_now, values_now, places_now = key_block(block_index)
        scores = block_scores(query_heads, keys_now, own_places, places_now, factor)
        newest = jnp.maximum(running, jnp.max(scores, axis=3))
        rescale = jnp.exp(running - newest)
        raised = jnp.exp(scores - newest[..., None])
        grad_probs = jnp.einsum(
            "qkgd,skd->kgqs", upstream_heads, values_now, preferred_element_type=jnp.float32
        )
        totals = totals * rescale + jnp.sum(raised, axis=3)
        delta_acc = delta_acc * rescale + jnp.sum(raised * grad_probs, axis=3)
        return ((newest, totals, delta_acc), None)

    start_stats = (
        jnp.full(stat_shape, -1e30, jnp.float32),
        jnp.zeros(stat_shape, jnp.float32),
        jnp.zeros(stat_shape, jnp.float32),
    )
    (running, totals, delta_acc), unused = lax.scan(stats_step, start_stats, block_ids)
    logsum = running + jnp.log(totals)
    deltas = delta_acc / totals

    def grad_pieces(block_index):
        keys_now, values_now, places_now = key_block(block_index)
        scores = block_scores(query_heads, keys_now, own_places, places_now, factor)
        weights = jnp.exp(scores - logsum[..., None])
        grad_probs = jnp.einsum(
            "qkgd,skd->kgqs", upstream_heads, values_now, preferred_element_type=jnp.float32
        )
        grad_scores = (weights * (grad_probs - deltas[..., None])).astype(jnp.bfloat16)
        return (keys_now, weights, grad_scores)

    query_zeros = jnp.zeros((own_rows, kv_heads, groups, HEAD_DIM), jnp.float32)

    def grad_step(carried, block_index):
        keys_now, weights, grad_scores = grad_pieces(block_index)
        carried = (
            carried
            + jnp.einsum(
                "kgqs,skd->qkgd", grad_scores, keys_now, preferred_element_type=jnp.float32
            )
            * factor
        )
        key_term = (
            jnp.einsum(
                "kgqs,qkgd->skd", grad_scores, query_heads, preferred_element_type=jnp.float32
            )
            * factor
        )
        value_term = jnp.einsum(
            "kgqs,qkgd->skd",
            weights.astype(jnp.bfloat16),
            upstream_heads,
            preferred_element_type=jnp.float32,
        )
        joined = jnp.concatenate(
            (key_term.reshape(block_rows, kv_width), value_term.reshape(block_rows, kv_width)),
            axis=1,
        )
        return (carried, joined)

    query_total, stacked = lax.scan(grad_step, query_zeros, block_ids)
    terms = stacked.reshape(seq_len, 2 * kv_width)
    mine = lax.psum_scatter(
        terms.astype(jnp.bfloat16), "cp", scatter_dimension=0, tiled=True
    ).astype(jnp.float32)
    key_grad = mine[:, :kv_width]
    value_grad = mine[:, kv_width:]
    query_grad = query_total.reshape(own_rows, kv_heads * groups * HEAD_DIM)
    return (query_grad, key_grad, value_grad)


MESH = pl.DeviceIdType.MESH
NT = (((1,), (1,)), ((), ()))
NN = (((1,), (0,)), ((), ()))
TILE = 256


def dot(a, b, dims):
    return lax.dot_general(a, b, dims, preferred_element_type=jnp.float32)


def greet(peers):
    barrier = pltpu.get_barrier_semaphore()
    for peer in peers:
        pl.semaphore_signal(barrier, inc=1, device_id=peer, device_id_type=MESH)
    pl.semaphore_wait(barrier, len(peers))


def send_kernel(
    n, kv_heads, q_ref, k_ref, v_ref, g_ref, w_ref, q_all, k_all, v_all, u_all,
    own_g, other_g, own_w, other_w, partial, u_buf,
    send_sem, recv_sem, q_sems, u_sems, own_sem, w_sem, g_sem, gx_sem,
):
    me = lax.axis_index("cp")
    half = lax.axis_index("vocab")
    mine = lax.rem(me, kv_heads)
    plane = me - mine
    width = g_ref.shape[1]
    wide = width // kv_heads
    cut = wide // 2
    offsets = list(range(kv_heads // 2, kv_heads)) + list(range(kv_heads // 2 - 1, -1, -1))
    steps = [(o, part) for o in offsets for part in range(2)]

    def member(o):
        return lax.rem(mine + o, kv_heads)

    def w_copy(t, own):
        o, part = steps[t]
        side = half if own else 1 - half
        return pltpu.make_async_copy(
            w_ref.at[
                pl.ds(pl.multiple_of(member(o) * wide + part * cut, cut), cut),
                pl.ds(pl.multiple_of(side * width, width), width),
            ],
            (own_w if own else other_w).at[t],
            w_sem.at[0 if own else 1, t],
        )

    own_g_copy = pltpu.make_async_copy(g_ref, own_g, g_sem)
    own_g_copy.start()
    for t in range(len(steps)):
        w_copy(t, True).start()
    for t in range(len(steps)):
        w_copy(t, False).start()

    greet([{"cp": lax.rem(me + s, n)} for s in range(1, n)] + [{"vocab": 1 - half}])

    g_copy = pltpu.make_async_remote_copy(
        src_ref=g_ref, dst_ref=other_g, send_sem=gx_sem.at[0], recv_sem=gx_sem.at[1],
        device_id={"vocab": 1 - half}, device_id_type=MESH,
    )
    g_copy.start()

    def columns(ref, at, size):
        return ref.at[:, pl.ds(pl.multiple_of(at * size, size), size)]

    def q_copy(o):
        to = member(o)
        return pltpu.make_async_remote_copy(
            src_ref=columns(q_ref, to, wide), dst_ref=q_all.at[mine],
            send_sem=q_sems.at[0, o], recv_sem=q_sems.at[1, o],
            device_id={"cp": plane + to}, device_id_type=MESH,
        )

    def u_copy(t):
        o, part = steps[t]
        return pltpu.make_async_remote_copy(
            src_ref=u_buf.at[t], dst_ref=u_all.at[mine, :, pl.ds(part * cut, cut)],
            send_sem=u_sems.at[0, t], recv_sem=u_sems.at[1, t],
            device_id={"cp": plane + member(o)}, device_id_type=MESH,
        )

    def kv_copies(s):
        peer = lax.rem(me + s, n)
        head = lax.rem(peer, kv_heads)
        return [
            pltpu.make_async_remote_copy(
                src_ref=columns(source, head, HEAD_DIM), dst_ref=target.at[me],
                send_sem=send_sem.at[i, s], recv_sem=recv_sem.at[i, s],
                device_id={"cp": peer}, device_id_type=MESH,
            )
            for i, (source, target) in enumerate(((k_ref, k_all), (v_ref, v_all)))
        ]

    def start_kv(s, carry):
        for copy in kv_copies(s):
            copy.start()
        return carry

    for o in offsets[:-1]:
        q_copy(o).start()
    lax.fori_loop(1, n, start_kv, 0)
    own_copies = [
        pltpu.make_async_copy(columns(q_ref, mine, wide), q_all.at[mine], own_sem.at[0]),
        pltpu.make_async_copy(columns(k_ref, mine, HEAD_DIM), k_all.at[me], own_sem.at[1]),
        pltpu.make_async_copy(columns(v_ref, mine, HEAD_DIM), v_all.at[me], own_sem.at[2]),
    ]
    for copy in own_copies:
        copy.start()

    own_g_copy.wait()
    for t in range(len(steps)):
        w_copy(t, True).wait()
        partial[t] = dot(own_g[...], own_w[t], NT)
    g_copy.wait()
    for t, (o, part) in enumerate(steps):
        w_copy(t, False).wait()
        block = (partial[t] + dot(other_g[...], other_w[t], NT)).astype(jnp.bfloat16)
        if o == 0:
            u_all[mine, :, pl.ds(part * cut, cut)] = block
        else:
            u_buf[t] = block
            u_copy(t).start()

    def wait_kv(s, carry):
        for copy in kv_copies(s):
            copy.wait()
        return carry

    lax.fori_loop(1, n, wait_kv, 0)
    for o in offsets[:-1]:
        q_copy(o).wait()
    for t, (o, part) in enumerate(steps):
        if o != 0:
            u_copy(t).wait()
    for copy in own_copies:
        copy.wait()


def attend_kernel(
    order_ref, q_ref, k_ref, v_ref, u_ref, dq_out, dkv_out,
    places, ks, vs, k_turned, s_buf, p_buf, dk_sum, dv_sum,
):
    plane = lax.axis_index("cp") // q_ref.shape[0]
    own_rows = q_ref.shape[1]
    groups = q_ref.shape[2] // HEAD_DIM
    seq = k_ref.shape[0]
    spans = order_ref.shape[0]
    rows = seq // spans
    tile = groups * rows
    own_spans = q_ref.shape[0] * own_rows // rows
    per_block = own_rows // rows
    factor = HEAD_DIM ** (-0.5)
    scale = factor * 1.4426950408889634

    for r in range(spans):
        places[order_ref[r]] = r
    for j in range(spans):
        source = pl.ds(pl.multiple_of(places[j] * rows, rows), rows)
        for target, ref in ((ks, k_ref), (vs, v_ref)):
            target[pl.ds(j * rows, rows), :] = ref[source, :]
    k_turned[...] = ks[...].T
    dk_sum[...] = jnp.zeros_like(dk_sum)
    dv_sum[...] = jnp.zeros_like(dv_sum)

    def fold(x, op):
        return op(x.reshape(TILE // 8, 8, tile), axis=0)

    key_at = lax.broadcasted_iota(jnp.int32, (TILE, tile), 0)
    query_at = lax.rem(lax.broadcasted_iota(jnp.int32, (TILE, tile), 1), rows)

    def one_span(t, carry):
        block = t // per_block
        own = pl.ds(pl.multiple_of(lax.rem(t, per_block) * rows, rows), rows)
        start = order_ref[plane * own_spans + t] * rows

        def stacked(ref):
            return jnp.concatenate(
                [ref[block, own, h * HEAD_DIM : (h + 1) * HEAD_DIM] for h in range(groups)], axis=0
            )

        def with_keys(last):
            q_tile = stacked(q_ref)
            u_tile = stacked(u_ref)
            peak = None
            for j in range(last + 1):
                keys = pl.ds(j * TILE, TILE)
                s = dot(ks[keys, :], q_tile, NT)
                if j == last:
                    s = jnp.where(key_at + (last * TILE - start) <= query_at, s, -1e30)
                s_buf[keys, :] = s
                top = fold(s, jnp.max)
                peak = top if peak is None else jnp.maximum(peak, top)
            peak = jnp.max(peak, axis=0, keepdims=True)
            total = jnp.zeros((8, tile), jnp.float32)
            delta = jnp.zeros((8, tile), jnp.float32)
            for j in range(last + 1):
                keys = pl.ds(j * TILE, TILE)
                p = jnp.exp2((s_buf[keys, :] - peak) * scale)
                dp = dot(vs[keys, :], u_tile, NT)
                total = total + fold(p, jnp.sum)
                delta = delta + fold(p * dp, jnp.sum)
                s_buf[keys, :] = p
                p_buf[keys, :] = dp
            inverse = 1.0 / jnp.sum(total, axis=0, keepdims=True)
            delta = jnp.sum(delta, axis=0, keepdims=True) * inverse
            turned = None
            for j in range(last + 1):
                keys = pl.ds(j * TILE, TILE)
                w = s_buf[keys, :] * inverse
                g = (w * (p_buf[keys, :] - delta)).astype(jnp.bfloat16)
                dk_sum[keys, :] += dot(g, q_tile, NN)
                dv_sum[keys, :] += dot(w.astype(jnp.bfloat16), u_tile, NN)
                part = dot(k_turned[:, keys], g, NN)
                turned = part if turned is None else turned + part
            dq = (turned.T * factor).astype(jnp.bfloat16)
            for h in range(groups):
                dq_out[block, own, h * HEAD_DIM : (h + 1) * HEAD_DIM] = dq[h * rows : (h + 1) * rows]

        for last in range(seq // TILE):
            pl.when(start // TILE == last)(functools.partial(with_keys, last))
        return carry

    lax.fori_loop(0, own_spans, one_span, 0)
    for r in range(spans):
        source = pl.ds(pl.multiple_of(order_ref[r] * rows, rows), rows)
        target = pl.ds(r * rows, rows)
        dkv_out[target, :HEAD_DIM] = (dk_sum[source, :] * factor).astype(jnp.bfloat16)
        dkv_out[target, HEAD_DIM:] = dv_sum[source, :].astype(jnp.bfloat16)


def return_kernel(n, kv_heads, dq_ref, dkv_ref, dq_all, dkv_all, send_sem, recv_sem, q_sems, own_sem):
    me = lax.axis_index("cp")
    mine = lax.rem(me, kv_heads)
    plane = me - mine
    wide = dq_ref.shape[2]
    greet([{"cp": lax.rem(me + s, n)} for s in range(1, n)])
    own_columns = pl.ds(pl.multiple_of(mine * wide, wide), wide)

    def dkv_copy(s):
        peer = lax.rem(me + s, n)
        return pltpu.make_async_remote_copy(
            src_ref=dkv_ref.at[peer], dst_ref=dkv_all.at[me],
            send_sem=send_sem.at[s], recv_sem=recv_sem.at[s],
            device_id={"cp": peer}, device_id_type=MESH,
        )

    def dq_copy(o):
        to = lax.rem(mine + o, kv_heads)
        return pltpu.make_async_remote_copy(
            src_ref=dq_ref.at[to], dst_ref=dq_all.at[:, own_columns],
            send_sem=q_sems.at[0, o], recv_sem=q_sems.at[1, o],
            device_id={"cp": plane + to}, device_id_type=MESH,
        )

    def start(s, carry):
        dkv_copy(s).start()
        return carry

    lax.fori_loop(1, n, start, 0)
    for o in range(1, kv_heads):
        dq_copy(o).start()
    own = (
        pltpu.make_async_copy(dkv_ref.at[me], dkv_all.at[me], own_sem.at[0]),
        pltpu.make_async_copy(dq_ref.at[mine], dq_all.at[:, own_columns], own_sem.at[1]),
    )
    for copy in own:
        copy.start()

    def wait(s, carry):
        dkv_copy(s).wait()
        return carry

    lax.fori_loop(1, n, wait, 0)
    for o in range(1, kv_heads):
        dq_copy(o).wait()
    for copy in own:
        copy.wait()


def by_planes(n, queries, key_states, value_states, out_grad, o_weight, span_order):
    own_rows, width = queries.shape
    kv_heads = key_states.shape[1] // HEAD_DIM
    wide = width // kv_heads
    cut = wide // 2
    seq = own_rows * n
    tile = (HEADS // KV_HEADS) * (seq // span_order.shape[0])
    hbm_spec = pl.BlockSpec(memory_space=pltpu.HBM)
    vmem_spec = pl.BlockSpec(memory_space=pltpu.VMEM)
    smem_spec = pl.BlockSpec(memory_space=pltpu.SMEM)
    dma = pltpu.SemaphoreType.DMA
    low = jnp.bfloat16
    q_block = jax.ShapeDtypeStruct((kv_heads, own_rows, wide), low)
    kv_block = jax.ShapeDtypeStruct((n, own_rows, HEAD_DIM), low)
    q_all, k_all, v_all, u_all = pl.pallas_call(
        functools.partial(send_kernel, n, kv_heads),
        out_shape=(q_block, kv_block, kv_block, q_block),
        in_specs=[hbm_spec] * 5,
        out_specs=(vmem_spec,) * 4,
        scratch_shapes=[
            pltpu.VMEM((own_rows, width), low),
            pltpu.VMEM((own_rows, width), low),
            pltpu.VMEM((2 * kv_heads, cut, width), low),
            pltpu.VMEM((2 * kv_heads, cut, width), low),
            pltpu.VMEM((2 * kv_heads, own_rows, cut), jnp.float32),
            pltpu.VMEM((2 * kv_heads, own_rows, cut), low),
            dma((2, n)),
            dma((2, n)),
            dma((2, kv_heads)),
            dma((2, 2 * kv_heads)),
            dma((3,)),
            dma((2, 2 * kv_heads)),
            dma(()),
            dma((2,)),
        ],
        compiler_params=pltpu.CompilerParams(
            collective_id=0, has_side_effects=True, vmem_limit_bytes=40 << 20
        ),
        name="send_heads",
    )(queries, key_states, value_states, out_grad, o_weight)
    dq, dkv = pl.pallas_call(
        attend_kernel,
        out_shape=(q_block, jax.ShapeDtypeStruct((seq, 2 * HEAD_DIM), low)),
        in_specs=[smem_spec] + [vmem_spec] * 4,
        out_specs=(vmem_spec,) * 2,
        scratch_shapes=[pltpu.SMEM(span_order.shape, jnp.int32)]
        + [pltpu.VMEM((seq, HEAD_DIM), low)] * 2
        + [pltpu.VMEM((HEAD_DIM, seq), low)]
        + [pltpu.VMEM((seq, tile), jnp.float32)] * 2
        + [pltpu.VMEM((seq, HEAD_DIM), jnp.float32)] * 2,
        compiler_params=pltpu.CompilerParams(vmem_limit_bytes=40 << 20),
        name="attend",
    )(span_order, q_all, k_all.reshape(seq, HEAD_DIM), v_all.reshape(seq, HEAD_DIM), u_all)
    dq_all, dkv_all = pl.pallas_call(
        functools.partial(return_kernel, n, kv_heads),
        out_shape=(
            jax.ShapeDtypeStruct((own_rows, width), low),
            jax.ShapeDtypeStruct((n, own_rows, 2 * HEAD_DIM), low),
        ),
        in_specs=[pl.BlockSpec(memory_space=pl.ANY)] * 2,
        out_specs=(vmem_spec,) * 2,
        scratch_shapes=[dma((n,)), dma((n,)), dma((2, kv_heads)), dma((2,))],
        compiler_params=pltpu.CompilerParams(
            collective_id=1, has_side_effects=True, vmem_limit_bytes=16 << 20
        ),
        name="return_grads",
    )(dq, dkv.reshape(n, own_rows, 2 * HEAD_DIM))

    def over_planes(part):
        heads = [
            sum(part[d].astype(jnp.float32) for d in range(g, n, kv_heads)) for g in range(kv_heads)
        ]
        return jnp.concatenate(heads, axis=1)

    return (
        dq_all.astype(jnp.float32),
        over_planes(dkv_all[:, :, :HEAD_DIM]),
        over_planes(dkv_all[:, :, HEAD_DIM:]),
    )


def solution(mesh):
    n = mesh.shape["cp"]
    planes = mesh.shape["vocab"] == 2 and n % (KV_HEADS // 2) == 0
    body = functools.partial(by_planes, n) if planes else local
    return jax.shard_map(
        body,
        mesh=mesh,
        in_specs=(
            P("cp", "vocab"),
            P("cp", "vocab"),
            P("cp", "vocab"),
            P("cp", "vocab"),
            P("vocab", None),
            P(),
        ),
        out_specs=(P("cp", "vocab"), P("cp", "vocab"), P("cp", "vocab")),
        check_vma=False,
    )
```

```python
import functools

import jax
import jax.numpy as jnp
from jax import lax
from jax.experimental import pallas as pl
from jax.experimental.pallas import tpu as pltpu
from jax.sharding import PartitionSpec as P

HEADS = 32
KV_HEADS = 8
HEAD_DIM = 128


def positions(span_order, span_rows):
    offsets = jnp.arange(span_rows, dtype=jnp.int32)
    return (span_order[:, None] * span_rows + offsets[None, :]).reshape(-1)


def block_scores(query_block, key_block, query_places, key_places, factor):
    scores = (
        jnp.einsum("qkgd,skd->kgqs", query_block, key_block, preferred_element_type=jnp.float32)
        * factor
    )
    visible = key_places[None, :] <= query_places[:, None]
    return jnp.where(visible, scores, -jnp.inf)


def local(queries, key_states, value_states, out_grad, o_weight, span_order):
    own_rows = queries.shape[0]
    kv_width = key_states.shape[1]
    kv_heads = kv_width // HEAD_DIM
    groups = HEADS // KV_HEADS
    factor = HEAD_DIM ** (-0.5)
    upstream = lax.dot_general(
        lax.all_gather(out_grad, "vocab", axis=1, tiled=True),
        o_weight,
        (((1,), (1,)), ((), ())),
        preferred_element_type=jnp.float32,
    ).astype(jnp.bfloat16)
    places = positions(span_order, own_rows // 2)
    seq_len = places.shape[0]
    own_places = lax.dynamic_slice_in_dim(places, lax.axis_index("cp") * own_rows, own_rows, 0)
    query_heads = queries.reshape(own_rows, kv_heads, groups, HEAD_DIM)
    upstream_heads = upstream.reshape(own_rows, kv_heads, groups, HEAD_DIM)
    key_all, value_all = (
        lax.all_gather(key_states, "cp", axis=0, tiled=True),
        lax.all_gather(value_states, "cp", axis=0, tiled=True),
    )
    key_all = key_all.reshape(seq_len, kv_heads, HEAD_DIM)
    value_all = value_all.reshape(seq_len, kv_heads, HEAD_DIM)
    block_rows = own_rows * 8
    block_count = seq_len // block_rows
    block_ids = jnp.arange(block_count, dtype=jnp.int32)
    stat_shape = (kv_heads, groups, own_rows)

    def key_block(block_index):
        offset = block_index * block_rows
        return (
            lax.dynamic_slice_in_dim(key_all, offset, block_rows, 0),
            lax.dynamic_slice_in_dim(value_all, offset, block_rows, 0),
            lax.dynamic_slice_in_dim(places, offset, block_rows, 0),
        )

    def stats_step(carried, block_index):
        running, totals, delta_acc = carried
        keys_now, values_now, places_now = key_block(block_index)
        scores = block_scores(query_heads, keys_now, own_places, places_now, factor)
        newest = jnp.maximum(running, jnp.max(scores, axis=3))
        rescale = jnp.exp(running - newest)
        raised = jnp.exp(scores - newest[..., None])
        grad_probs = jnp.einsum(
            "qkgd,skd->kgqs", upstream_heads, values_now, preferred_element_type=jnp.float32
        )
        totals = totals * rescale + jnp.sum(raised, axis=3)
        delta_acc = delta_acc * rescale + jnp.sum(raised * grad_probs, axis=3)
        return ((newest, totals, delta_acc), None)

    start_stats = (
        jnp.full(stat_shape, -1e30, jnp.float32),
        jnp.zeros(stat_shape, jnp.float32),
        jnp.zeros(stat_shape, jnp.float32),
    )
    (running, totals, delta_acc), unused = lax.scan(stats_step, start_stats, block_ids)
    logsum = running + jnp.log(totals)
    deltas = delta_acc / totals

    def grad_pieces(block_index):
        keys_now, values_now, places_now = key_block(block_index)
        scores = block_scores(query_heads, keys_now, own_places, places_now, factor)
        weights = jnp.exp(scores - logsum[..., None])
        grad_probs = jnp.einsum(
            "qkgd,skd->kgqs", upstream_heads, values_now, preferred_element_type=jnp.float32
        )
        grad_scores = (weights * (grad_probs - deltas[..., None])).astype(jnp.bfloat16)
        return (keys_now, weights, grad_scores)

    query_zeros = jnp.zeros((own_rows, kv_heads, groups, HEAD_DIM), jnp.float32)

    def grad_step(carried, block_index):
        keys_now, weights, grad_scores = grad_pieces(block_index)
        carried = (
            carried
            + jnp.einsum(
                "kgqs,skd->qkgd", grad_scores, keys_now, preferred_element_type=jnp.float32
            )
            * factor
        )
        key_term = (
            jnp.einsum(
                "kgqs,qkgd->skd", grad_scores, query_heads, preferred_element_type=jnp.float32
            )
            * factor
        )
        value_term = jnp.einsum(
            "kgqs,qkgd->skd",
            weights.astype(jnp.bfloat16),
            upstream_heads,
            preferred_element_type=jnp.float32,
        )
        joined = jnp.concatenate(
            (key_term.reshape(block_rows, kv_width), value_term.reshape(block_rows, kv_width)),
            axis=1,
        )
        return (carried, joined)

    query_total, stacked = lax.scan(grad_step, query_zeros, block_ids)
    terms = stacked.reshape(seq_len, 2 * kv_width)
    mine = lax.psum_scatter(
        terms.astype(jnp.bfloat16), "cp", scatter_dimension=0, tiled=True
    ).astype(jnp.float32)
    key_grad = mine[:, :kv_width]
    value_grad = mine[:, kv_width:]
    query_grad = query_total.reshape(own_rows, kv_heads * groups * HEAD_DIM)
    return (query_grad, key_grad, value_grad)


MESH = pl.DeviceIdType.MESH
NT = (((1,), (1,)), ((), ()))
NN = (((1,), (0,)), ((), ()))
TILE = 256


def dot(a, b, dims):
    return lax.dot_general(a, b, dims, preferred_element_type=jnp.float32)


def greet(peers):
    barrier = pltpu.get_barrier_semaphore()
    for peer in peers:
        pl.semaphore_signal(barrier, inc=1, device_id=peer, device_id_type=MESH)
    pl.semaphore_wait(barrier, len(peers))


def send_kernel(
    n, kv_heads, q_ref, k_ref, v_ref, g_ref, w_ref, q_all, k_all, v_all, u_all,
    own_g, other_g, own_w, other_w, partial, u_buf,
    send_sem, recv_sem, q_sems, u_sems, own_sem, w_sem, g_sem, gx_sem,
):
    me = lax.axis_index("cp")
    half = lax.axis_index("vocab")
    mine = lax.rem(me, kv_heads)
    plane = me - mine
    width = g_ref.shape[1]
    wide = width // kv_heads
    cut = wide // 2
    offsets = list(range(kv_heads // 2, kv_heads)) + list(range(kv_heads // 2 - 1, -1, -1))
    steps = [(o, part) for o in offsets for part in range(2)]

    def member(o):
        return lax.rem(mine + o, kv_heads)

    def w_copy(t, own):
        o, part = steps[t]
        side = half if own else 1 - half
        return pltpu.make_async_copy(
            w_ref.at[
                pl.ds(pl.multiple_of(member(o) * wide + part * cut, cut), cut),
                pl.ds(pl.multiple_of(side * width, width), width),
            ],
            (own_w if own else other_w).at[t],
            w_sem.at[0 if own else 1, t],
        )

    own_g_copy = pltpu.make_async_copy(g_ref, own_g, g_sem)
    own_g_copy.start()
    for t in range(len(steps)):
        w_copy(t, True).start()
    for t in range(len(steps)):
        w_copy(t, False).start()

    greet([{"cp": lax.rem(me + s, n)} for s in range(1, n)] + [{"vocab": 1 - half}])

    g_copy = pltpu.make_async_remote_copy(
        src_ref=g_ref, dst_ref=other_g, send_sem=gx_sem.at[0], recv_sem=gx_sem.at[1],
        device_id={"vocab": 1 - half}, device_id_type=MESH,
    )
    g_copy.start()

    def columns(ref, at, size):
        return ref.at[:, pl.ds(pl.multiple_of(at * size, size), size)]

    def q_copy(o):
        to = member(o)
        return pltpu.make_async_remote_copy(
            src_ref=columns(q_ref, to, wide), dst_ref=q_all.at[mine],
            send_sem=q_sems.at[0, o], recv_sem=q_sems.at[1, o],
            device_id={"cp": plane + to}, device_id_type=MESH,
        )

    def u_copy(t):
        o, part = steps[t]
        return pltpu.make_async_remote_copy(
            src_ref=u_buf.at[t], dst_ref=u_all.at[mine, :, pl.ds(part * cut, cut)],
            send_sem=u_sems.at[0, t], recv_sem=u_sems.at[1, t],
            device_id={"cp": plane + member(o)}, device_id_type=MESH,
        )

    def kv_copies(s):
        peer = lax.rem(me + s, n)
        head = lax.rem(peer, kv_heads)
        return [
            pltpu.make_async_remote_copy(
                src_ref=columns(source, head, HEAD_DIM), dst_ref=target.at[me],
                send_sem=send_sem.at[i, s], recv_sem=recv_sem.at[i, s],
                device_id={"cp": peer}, device_id_type=MESH,
            )
            for i, (source, target) in enumerate(((k_ref, k_all), (v_ref, v_all)))
        ]

    def start_kv(s, carry):
        for copy in kv_copies(s):
            copy.start()
        return carry

    for o in offsets[:-1]:
        q_copy(o).start()
    lax.fori_loop(1, n, start_kv, 0)
    own_copies = [
        pltpu.make_async_copy(columns(q_ref, mine, wide), q_all.at[mine], own_sem.at[0]),
        pltpu.make_async_copy(columns(k_ref, mine, HEAD_DIM), k_all.at[me], own_sem.at[1]),
        pltpu.make_async_copy(columns(v_ref, mine, HEAD_DIM), v_all.at[me], own_sem.at[2]),
    ]
    for copy in own_copies:
        copy.start()

    own_g_copy.wait()
    for t in range(len(steps)):
        w_copy(t, True).wait()
        partial[t] = dot(own_g[...], own_w[t], NT)
    g_copy.wait()
    for t, (o, part) in enumerate(steps):
        w_copy(t, False).wait()
        block = (partial[t] + dot(other_g[...], other_w[t], NT)).astype(jnp.bfloat16)
        if o == 0:
            u_all[mine, :, pl.ds(part * cut, cut)] = block
        else:
            u_buf[t] = block
            u_copy(t).start()

    def wait_kv(s, carry):
        for copy in kv_copies(s):
            copy.wait()
        return carry

    lax.fori_loop(1, n, wait_kv, 0)
    for o in offsets[:-1]:
        q_copy(o).wait()
    for t, (o, part) in enumerate(steps):
        if o != 0:
            u_copy(t).wait()
    for copy in own_copies:
        copy.wait()


def attend_kernel(
    order_ref, q_ref, k_ref, v_ref, u_ref, dq_out, dkv_out,
    places, ks, vs, k_turned, s_buf, p_buf, dk_sum, dv_sum,
):
    plane = lax.axis_index("cp") // q_ref.shape[0]
    own_rows = q_ref.shape[1]
    groups = q_ref.shape[2] // HEAD_DIM
    seq = k_ref.shape[0]
    spans = order_ref.shape[0]
    rows = seq // spans
    tile = groups * rows
    own_spans = q_ref.shape[0] * own_rows // rows
    per_block = own_rows // rows
    factor = HEAD_DIM ** (-0.5)
    scale = factor * 1.4426950408889634

    for r in range(spans):
        places[order_ref[r]] = r
    for j in range(spans):
        source = pl.ds(pl.multiple_of(places[j] * rows, rows), rows)
        for target, ref in ((ks, k_ref), (vs, v_ref)):
            target[pl.ds(j * rows, rows), :] = ref[source, :]
    k_turned[...] = ks[...].T
    dk_sum[...] = jnp.zeros_like(dk_sum)
    dv_sum[...] = jnp.zeros_like(dv_sum)

    def fold(x, op):
        return op(x.reshape(TILE // 8, 8, tile), axis=0)

    key_at = lax.broadcasted_iota(jnp.int32, (TILE, tile), 0)
    query_at = lax.rem(lax.broadcasted_iota(jnp.int32, (TILE, tile), 1), rows)

    def one_span(t, carry):
        block = t // per_block
        own = pl.ds(pl.multiple_of(lax.rem(t, per_block) * rows, rows), rows)
        start = order_ref[plane * own_spans + t] * rows

        def stacked(ref):
            return jnp.concatenate(
                [ref[block, own, h * HEAD_DIM : (h + 1) * HEAD_DIM] for h in range(groups)], axis=0
            )

        def with_keys(last):
            q_tile = stacked(q_ref)
            u_tile = stacked(u_ref)
            peak = None
            for j in range(last + 1):
                keys = pl.ds(j * TILE, TILE)
                s = dot(ks[keys, :], q_tile, NT)
                if j == last:
                    s = jnp.where(key_at + (last * TILE - start) <= query_at, s, -1e30)
                s_buf[keys, :] = s
                top = fold(s, jnp.max)
                peak = top if peak is None else jnp.maximum(peak, top)
            peak = jnp.max(peak, axis=0, keepdims=True)
            total = jnp.zeros((8, tile), jnp.float32)
            delta = jnp.zeros((8, tile), jnp.float32)
            for j in range(last + 1):
                keys = pl.ds(j * TILE, TILE)
                p = jnp.exp2((s_buf[keys, :] - peak) * scale)
                dp = dot(vs[keys, :], u_tile, NT)
                total = total + fold(p, jnp.sum)
                delta = delta + fold(p * dp, jnp.sum)
                s_buf[keys, :] = p
                p_buf[keys, :] = dp
            inverse = 1.0 / jnp.sum(total, axis=0, keepdims=True)
            delta = jnp.sum(delta, axis=0, keepdims=True) * inverse
            turned = None
            for j in range(last + 1):
                keys = pl.ds(j * TILE, TILE)
                w = s_buf[keys, :] * inverse
                g = (w * (p_buf[keys, :] - delta)).astype(jnp.bfloat16)
                dk_sum[keys, :] += dot(g, q_tile, NN)
                dv_sum[keys, :] += dot(w.astype(jnp.bfloat16), u_tile, NN)
                part = dot(k_turned[:, keys], g, NN)
                turned = part if turned is None else turned + part
            dq = (turned.T * factor).astype(jnp.bfloat16)
            for h in range(groups):
                dq_out[block, own, h * HEAD_DIM : (h + 1) * HEAD_DIM] = dq[h * rows : (h + 1) * rows]

        for last in range(seq // TILE):
            pl.when(start // TILE == last)(functools.partial(with_keys, last))
        return carry

    lax.fori_loop(0, own_spans, one_span, 0)
    for r in range(spans):
        source = pl.ds(pl.multiple_of(order_ref[r] * rows, rows), rows)
        target = pl.ds(r * rows, rows)
        dkv_out[target, :HEAD_DIM] = (dk_sum[source, :] * factor).astype(jnp.bfloat16)
        dkv_out[target, HEAD_DIM:] = dv_sum[source, :].astype(jnp.bfloat16)


def return_kernel(
    kv_heads, dq_ref, dkv_ref, dq_all, dkv_all,
    relay, summed, send_sem, recv_sem, relay_sems, q_sems, own_sem,
):
    me = lax.axis_index("cp")
    mine = lax.rem(me, kv_heads)
    plane = me // kv_heads
    pair = plane + 1 - 2 * lax.rem(plane, 2)
    across = lax.rem(plane + 2, 4)
    pair_across = lax.rem(pair + 2, 4)
    wide = dq_ref.shape[2]
    n = 4 * kv_heads
    greet([{"cp": lax.rem(me + s, n)} for s in range(1, n)])
    own_columns = pl.ds(pl.multiple_of(mine * wide, wide), wide)

    def relay_copy(m):
        return pltpu.make_async_remote_copy(
            src_ref=dkv_ref.at[pair_across * kv_heads + m], dst_ref=relay.at[m],
            send_sem=relay_sems.at[0, m], recv_sem=relay_sems.at[1, m],
            device_id={"cp": pair * kv_heads + mine}, device_id_type=MESH,
        )

    def dkv_copy(kind, m, source):
        to = (plane, pair, across)[kind] * kv_heads + m
        return pltpu.make_async_remote_copy(
            src_ref=dkv_ref.at[to] if source is None else source,
            dst_ref=dkv_all.at[kind * kv_heads + mine],
            send_sem=send_sem.at[kind, m], recv_sem=recv_sem.at[kind, mine],
            device_id={"cp": to}, device_id_type=MESH,
        )

    def arrived(kind, g):
        slot = dkv_all.at[kind * kv_heads + g]
        pltpu.make_async_remote_copy(
            src_ref=slot, dst_ref=slot,
            send_sem=send_sem.at[kind, g], recv_sem=recv_sem.at[kind, g],
            device_id={"cp": pair * kv_heads + mine}, device_id_type=MESH,
        ).wait_recv()

    def dq_copy(o):
        to = lax.rem(mine + o, kv_heads)
        return pltpu.make_async_remote_copy(
            src_ref=dq_ref.at[to], dst_ref=dq_all.at[:, own_columns],
            send_sem=q_sems.at[0, o], recv_sem=q_sems.at[1, o],
            device_id={"cp": plane * kv_heads + to}, device_id_type=MESH,
        )

    others = [lax.rem(mine + o, kv_heads) for o in range(1, kv_heads)]
    for m in range(kv_heads):
        relay_copy(m).start()
    for o in range(1, kv_heads):
        dq_copy(o).start()
    own = pltpu.make_async_copy(dq_ref.at[mine], dq_all.at[:, own_columns], own_sem)
    own.start()
    for m in range(kv_heads):
        relay_copy(m).wait_recv()
        total = dkv_ref[across * kv_heads + m].astype(jnp.float32) + relay[m].astype(jnp.float32)
        summed[m] = total.astype(jnp.bfloat16)
        dkv_copy(2, m, summed.at[m]).start()
        dkv_copy(1, m, None).start()
    for m in others:
        dkv_copy(0, m, None).start()
    dkv_all[mine] = dkv_ref[me]

    for m in range(kv_heads):
        relay_copy(m).wait_send()
        dkv_copy(2, m, summed.at[m]).wait_send()
        dkv_copy(1, m, None).wait_send()
        arrived(1, m)
        arrived(2, m)
    for m in others:
        dkv_copy(0, m, None).wait_send()
        arrived(0, m)
    for o in range(1, kv_heads):
        dq_copy(o).wait()
    own.wait()


def by_planes(n, queries, key_states, value_states, out_grad, o_weight, span_order):
    own_rows, width = queries.shape
    kv_heads = key_states.shape[1] // HEAD_DIM
    wide = width // kv_heads
    cut = wide // 2
    seq = own_rows * n
    tile = (HEADS // KV_HEADS) * (seq // span_order.shape[0])
    hbm_spec = pl.BlockSpec(memory_space=pltpu.HBM)
    vmem_spec = pl.BlockSpec(memory_space=pltpu.VMEM)
    smem_spec = pl.BlockSpec(memory_space=pltpu.SMEM)
    dma = pltpu.SemaphoreType.DMA
    low = jnp.bfloat16
    q_block = jax.ShapeDtypeStruct((kv_heads, own_rows, wide), low)
    kv_block = jax.ShapeDtypeStruct((n, own_rows, HEAD_DIM), low)
    q_all, k_all, v_all, u_all = pl.pallas_call(
        functools.partial(send_kernel, n, kv_heads),
        out_shape=(q_block, kv_block, kv_block, q_block),
        in_specs=[hbm_spec] * 5,
        out_specs=(vmem_spec,) * 4,
        scratch_shapes=[
            pltpu.VMEM((own_rows, width), low),
            pltpu.VMEM((own_rows, width), low),
            pltpu.VMEM((2 * kv_heads, cut, width), low),
            pltpu.VMEM((2 * kv_heads, cut, width), low),
            pltpu.VMEM((2 * kv_heads, own_rows, cut), jnp.float32),
            pltpu.VMEM((2 * kv_heads, own_rows, cut), low),
            dma((2, n)),
            dma((2, n)),
            dma((2, kv_heads)),
            dma((2, 2 * kv_heads)),
            dma((3,)),
            dma((2, 2 * kv_heads)),
            dma(()),
            dma((2,)),
        ],
        compiler_params=pltpu.CompilerParams(
            collective_id=0, has_side_effects=True, vmem_limit_bytes=40 << 20
        ),
        name="send_heads",
    )(queries, key_states, value_states, out_grad, o_weight)
    dq, dkv = pl.pallas_call(
        attend_kernel,
        out_shape=(q_block, jax.ShapeDtypeStruct((seq, 2 * HEAD_DIM), low)),
        in_specs=[smem_spec] + [vmem_spec] * 4,
        out_specs=(vmem_spec,) * 2,
        scratch_shapes=[pltpu.SMEM(span_order.shape, jnp.int32)]
        + [pltpu.VMEM((seq, HEAD_DIM), low)] * 2
        + [pltpu.VMEM((HEAD_DIM, seq), low)]
        + [pltpu.VMEM((seq, tile), jnp.float32)] * 2
        + [pltpu.VMEM((seq, HEAD_DIM), jnp.float32)] * 2,
        compiler_params=pltpu.CompilerParams(vmem_limit_bytes=40 << 20),
        name="attend",
    )(span_order, q_all, k_all.reshape(seq, HEAD_DIM), v_all.reshape(seq, HEAD_DIM), u_all)
    term = (own_rows, 2 * HEAD_DIM)
    dq_all, dkv_all = pl.pallas_call(
        functools.partial(return_kernel, kv_heads),
        out_shape=(
            jax.ShapeDtypeStruct((own_rows, width), low),
            jax.ShapeDtypeStruct((3 * kv_heads,) + term, low),
        ),
        in_specs=[pl.BlockSpec(memory_space=pl.ANY), vmem_spec],
        out_specs=(vmem_spec,) * 2,
        scratch_shapes=[pltpu.VMEM((kv_heads,) + term, low)] * 2
        + [
            dma((3, kv_heads)),
            dma((3, kv_heads)),
            dma((2, kv_heads)),
            dma((2, kv_heads)),
            dma(()),
        ],
        compiler_params=pltpu.CompilerParams(
            collective_id=1, has_side_effects=True, vmem_limit_bytes=16 << 20
        ),
        name="return_grads",
    )(dq, dkv.reshape((n,) + term))

    def over_planes(part):
        heads = [
            sum(part[d].astype(jnp.float32) for d in range(g, 3 * kv_heads, kv_heads)) for g in range(kv_heads)
        ]
        return jnp.concatenate(heads, axis=1)

    return (
        dq_all.astype(jnp.float32),
        over_planes(dkv_all[:, :, :HEAD_DIM]),
        over_planes(dkv_all[:, :, HEAD_DIM:]),
    )


def solution(mesh):
    n = mesh.shape["cp"]
    planes = mesh.shape["vocab"] == 2 and n == 4 * (KV_HEADS // 2)
    body = functools.partial(by_planes, n) if planes else local
    return jax.shard_map(
        body,
        mesh=mesh,
        in_specs=(
            P("cp", "vocab"),
            P("cp", "vocab"),
            P("cp", "vocab"),
            P("cp", "vocab"),
            P("vocab", None),
            P(),
        ),
        out_specs=(P("cp", "vocab"), P("cp", "vocab"), P("cp", "vocab")),
        check_vma=False,
    )
```
